64 devices in a mesh: rep: 8 (over x, y, core), dp: 8 (over z).
Axes of the slice: x: 2, y: 2, z: 8, core: 2. Of those that a mesh axis runs over, the one named last changes fastest.
The devices are a block of a 4x4x8 slice.
Arguments:
- x: bfloat16 [64, 4096, 512], P(('rep', 'dp')), parts along dimension 0
- dy: bfloat16 [64, 4096, 512], P(('rep', 'dp')), parts along dimension 0
- w_gate: bfloat16 [2, 512, 1664], replicated
- w_up: bfloat16 [2, 512, 1664], replicated
- w_down: bfloat16 [2, 1664, 512], replicated
- m_w_gate: float32 [2, 512, 1664], replicated
- m_w_up: float32 [2, 512, 1664], replicated
- m_w_down: float32 [2, 1664, 512], replicated
- v_w_gate: float32 [2, 512, 1664], replicated
- v_w_up: float32 [2, 512, 1664], replicated
- v_w_down: float32 [2, 1664, 512], replicated
Outputs:
- output 1: bfloat16 [16, 512, 1664], P('rep'), parts along dimension 0
- output 2: bfloat16 [16, 512, 1664], P('rep'), parts along dimension 0
- output 3: bfloat16 [16, 1664, 512], P('rep'), parts along dimension 0
- output 4: float32 [16, 512, 1664], P('rep'), parts along dimension 0
- output 5: float32 [16, 512, 1664], P('rep'), parts along dimension 0
- output 6: float32 [16, 1664, 512], P('rep'), parts along dimension 0
- output 7: float32 [16, 512, 1664], P('rep'), parts along dimension 0
- output 8: float32 [16, 512, 1664], P('rep'), parts along dimension 0
- output 9: float32 [16, 1664, 512], P('rep'), parts along dimension 0
There are 8 independent parts. The reference program is written for one: setup_inputs(seed, part) draws one part's arguments, and reference() takes and returns one part's arrays. A program takes and returns all parts, laid end to end along the dimension named above; an argument that names none is the same for every part.
All inputs are finite; a program needn't handle non-finite values.
Results may differ from the reference program's by a relative error of at most 0.022.
Values are sent between devices in bfloat16 or wider.
A program may use at most 768 MiB of HBM per device.

```python
import jax
import jax.numpy as jnp
from jax import lax

SEQUENCES = 8
TOKENS = 4096
D = 512
FF = 1664
LAYERS = 2
NAMES = ("w_gate", "w_up", "w_down")
SHAPES = {"w_gate": (LAYERS, D, FF), "w_up": (LAYERS, D, FF), "w_down": (LAYERS, FF, D)}


def bump(key, n, height):
    away = (jnp.arange(n, dtype=jnp.int32) - jax.random.randint(key, (), 0, n, jnp.int32)) % n
    return jnp.where(away < n // 8, height, 1.0)


def together(key, own, strength):
    shared = jax.random.normal(key, own.shape[1:], jnp.float32)
    return (own + strength * shared) * lax.rsqrt(1 + strength * strength)


def setup_inputs(seed: int = 0, part: int = 0) -> dict:
    kx, kdy, ka, kb, kz, kf, kh, kl, *keys = jax.random.split(jax.random.key(seed), 8 + 3 * len(NAMES))
    kx, kdy, ka, kb = (jax.random.fold_in(k, part) for k in (kx, kdy, ka, kb))
    kw, km, kv = (keys[i::3] for i in range(3))
    shape = (SEQUENCES, TOKENS, D)
    much_x, much_dy = jax.random.uniform(kz, (2,), jnp.float32, 0.0, 1.0)
    loud = 2.0 ** jax.random.uniform(jax.random.fold_in(kz, 1), (), jnp.float32, -1.0, 2.0)
    layers = 2.0 ** jax.random.uniform(kl, (LAYERS, 1, 1), jnp.float32, -1.0, 1.0)
    x = together(ka, jax.random.normal(kx, shape, jnp.float32), much_x) * bump(kf, D, 4.0)
    dy = together(kb, jax.random.normal(kdy, shape, jnp.float32), much_dy)
    drawn = {"x": x.astype(jnp.bfloat16), "dy": (loud * dy * (SEQUENCES * TOKENS) ** -0.5).astype(jnp.bfloat16)}
    for key, name in zip(kw, NAMES, strict=True):
        w = jax.random.normal(key, SHAPES[name], jnp.float32) * SHAPES[name][1] ** -0.5
        drawn[name] = (w * {"w_gate": 1.0, "w_up": bump(kh, FF, 4.0), "w_down": layers}[name]).astype(jnp.bfloat16)
    for key, name in zip(km, NAMES, strict=True):
        drawn[f"m_{name}"] = 0.1 * jax.random.normal(key, SHAPES[name], jnp.float32)
    for key, name in zip(kv, NAMES, strict=True):
        drawn[f"v_{name}"] = jax.random.uniform(key, SHAPES[name], jnp.float32, 0.005, 0.015)
    return drawn


def matmul(a, w):
    return jnp.dot(a, w, preferred_element_type=jnp.float32).astype(jnp.bfloat16)


def normed(h):
    wide = h.astype(jnp.float32)
    scale = lax.rsqrt(jnp.mean(wide**2, -1, keepdims=True) + 1e-6)
    return (wide * scale).astype(jnp.bfloat16)


def layer(h, w):
    a = normed(h)
    gate = jnp.dot(a, w["w_gate"], preferred_element_type=jnp.float32)
    up = jnp.dot(a, w["w_up"], preferred_element_type=jnp.float32)
    return h + matmul((jax.nn.silu(gate) * up).astype(jnp.bfloat16), w["w_down"])


def adamw(w, m, v, g):
    m = 0.9 * m + 0.1 * g
    v = 0.95 * v + 0.05 * g * g
    step = m * lax.rsqrt(v + 1e-8) + 0.1 * w
    return (w - 0.02 * step).astype(jnp.bfloat16), m, v


def clipped(gradients, sum_of_squares, count):
    factor = jnp.minimum(1.0, 0.5 * lax.rsqrt(sum_of_squares / count + 1e-30))
    return [g * factor for g in gradients]


def stack(weights, h):
    return lax.scan(lambda h, w: (layer(h, w), None), h, weights)[0]


def reference(x, dy, w_gate, w_up, w_down, m_w_gate, m_w_up, m_w_down, v_w_gate, v_w_up, v_w_down):
    weights = dict(zip(NAMES, (w_gate, w_up, w_down), strict=True))

    def take(so_far, sequence):
        h, by_y = sequence
        _, back = jax.vjp(lambda w: stack(w, h), weights)
        return jax.tree.map(lambda total, term: total + term.astype(jnp.float32), so_far, back(by_y)[0]), None

    none_yet = {name: jnp.zeros(w.shape, jnp.float32) for name, w in weights.items()}
    by_weights, _ = lax.scan(take, none_yet, (x, dy))
    gradients = [by_weights[name].astype(jnp.bfloat16).astype(jnp.float32) for name in NAMES]
    gradients = clipped(gradients, sum(jnp.sum(g * g) for g in gradients), sum(g.size for g in gradients))
    new = [
        adamw(w.astype(jnp.float32), m, v, g)
        for w, m, v, g in zip((w_gate, w_up, w_down), (m_w_gate, m_w_up, m_w_down), (v_w_gate, v_w_up, v_w_down), gradients, strict=True)
    ]
    return tuple(one[which] for which in range(3) for one in new)
```

```python
import functools

import jax
import jax.numpy as jnp
from jax import lax
from jax.experimental import pallas as pl
from jax.experimental.pallas import tpu as pltpu
from jax.sharding import PartitionSpec as P

MESH = pl.DeviceIdType.MESH
LANES = 128
KINDS = 3
WIDE = 2
SLOTS = 4
F32, BF16 = jnp.float32, jnp.bfloat16


def nn(a, b):
    return lax.dot_general(a, b, (((1,), (0,)), ((), ())), preferred_element_type=F32)


def nt(a, b):
    return lax.dot_general(a, b, (((1,), (1,)), ((), ())), preferred_element_type=F32)


def tn(a, b):
    return lax.dot_general(a, b, (((0,), (0,)), ((), ())), preferred_element_type=F32)


def sigmoid(x):
    return 0.5 * jnp.tanh(0.5 * x) + 0.5


def normed(h):
    wide = h.astype(F32)
    scale = lax.rsqrt(jnp.mean(wide * wide, -1, keepdims=True) + 1e-6)
    return (wide * scale).astype(BF16)


def normed_back(h, da):
    wide, da = h.astype(F32), da.astype(BF16).astype(F32)
    scale = lax.rsqrt(jnp.mean(wide * wide, -1, keepdims=True) + 1e-6)
    return (scale * (da - wide * (scale * scale * jnp.mean(da * wide, -1, keepdims=True)))).astype(BF16)


def gradients_kernel(
    n, x_hbm, dy_hbm, wg_hbm, wu_hbm, wd_hbm, g_hbm, squares_ref,
    a0, h1, a1, dh, wg, wu, wd, da, acc, part, recv, own_squares, all_squares,
    load_x, load_dy, load_w, send_sem, recv_sem, keep_sem, sq_send, sq_recv,
):
    tokens, d = x_hbm.shape
    ff = wg.shape[-1]
    blocks = ff // LANES
    per_layer = (blocks + 1) // WIDE
    pieces = 2 * per_layer
    rows = KINDS * LANES // n
    tiles = load_x.shape[0]
    tile = tokens // tiles
    me = lax.axis_index("dp")

    def load_tile(hbm, ref, sem, i):
        at = pl.ds(pl.multiple_of(i * tile, tile), tile)
        return pltpu.make_async_copy(hbm.at[at], ref.at[at], sem.at[i])

    def load_weight(i, layer):
        hbm, ref = ((wg_hbm, wg), (wu_hbm, wu), (wd_hbm, wd))[i]
        return pltpu.make_async_copy(hbm.at[layer], ref.at[layer], load_w.at[layer, i])

    load_tile(x_hbm, a0, load_x, 0).start()
    for i in range(KINDS):
        load_weight(i, 0).start()
    for i in range(1, tiles):
        load_tile(x_hbm, a0, load_x, i).start()
    for i in range(KINDS):
        load_weight(i, 1).start()
    for i in range(tiles):
        load_tile(dy_hbm, dh, load_dy, i).start()

    barrier = pltpu.get_barrier_semaphore()
    for away in range(1, n):
        pl.semaphore_signal(barrier, inc=1, device_id={"dp": lax.rem(me + away, n)}, device_id_type=MESH)
    pl.semaphore_wait(barrier, n - 1)

    own_squares[...] = jnp.zeros_like(own_squares)

    for i in range(KINDS):
        load_weight(i, 0).wait()
    bounds = [(f, min(f + 2 * LANES, ff)) for f in range(0, ff, 2 * LANES)]

    def forward(i, _):
        load_tile(x_hbm, a0, load_x, i).wait()
        at = pl.ds(pl.multiple_of(i * tile, tile), tile)
        h = a0[at]
        a = normed(h)
        total = None
        for lo, hi in bounds:
            gate, up = nn(a, wg[0, :, lo:hi]), nn(a, wu[0, :, lo:hi])
            y = nn((gate * sigmoid(gate) * up).astype(BF16), wd[0, lo:hi, :])
            total = y if total is None else total + y
        h = (h.astype(F32) + total.astype(BF16).astype(F32)).astype(BF16)
        a0[at] = a
        h1[at] = h
        a1[at] = normed(h)
        da[at] = jnp.zeros((tile, d), F32)
        return 0

    lax.fori_loop(0, tiles, forward, 0)
    for i in range(KINDS):
        load_weight(i, 1).wait()
    for i in range(tiles):
        load_tile(dy_hbm, dh, load_dy, i).wait()

    def chunk(c):
        return pl.ds(pl.multiple_of(lax.rem(c + 2 * n, n) * rows, rows), rows)

    def copy_of(p, way, age, kind):
        block, sign = WIDE * p + way, 1 - 2 * way
        if kind == "sum":
            source = part.at[block, chunk(me - sign * (age + 1))]
            target = recv.at[block, age]
        else:
            at = chunk(me - sign * (age - (n - 1)))
            source = part.at[block, at] if kind == "first" else g_hbm.at[block, at]
            target = g_hbm.at[block, at]
        return pltpu.make_async_remote_copy(
            src_ref=source,
            dst_ref=target,
            send_sem=send_sem.at[block],
            recv_sem=recv_sem.at[block, age],
            device_id={"dp": lax.rem(me + sign + n, n)},
            device_id_type=MESH,
        )

    def arrived(p, way, age, kind):
        copy = copy_of(p, way, age, kind)
        copy.wait_send()
        if kind == "sum":
            copy.wait_recv()
        else:
            block, sign = WIDE * p + way, 1 - 2 * way
            at = chunk(me - sign * (age - (n - 1) + 1))
            pltpu.make_async_remote_copy(
                src_ref=g_hbm.at[block, at],
                dst_ref=g_hbm.at[block, at],
                send_sem=send_sem.at[block],
                recv_sem=recv_sem.at[block, age],
                device_id={"dp": lax.rem(me + sign + n, n)},
                device_id_type=MESH,
            ).wait_recv()

    def add(p, way, age):
        block, sign = WIDE * p + way, 1 - 2 * way
        at = chunk(me - sign * (age + 1))
        total = (part[block, at].astype(F32) + recv[block, age - 1].astype(F32)).astype(BF16)
        part[block, at] = total
        return total

    def keep(p, way):
        block = WIDE * p + way
        return pltpu.make_async_copy(part.at[block, chunk(me)], g_hbm.at[block, chunk(me)], keep_sem.at[block])

    def finish(p, way):
        total = add(p, way, n - 1).astype(F32)
        copy_of(p, way, n - 1, "first").start()
        keep(p, way).start()
        total = total * total
        squares = own_squares[...]
        for r in range(0, rows, 8):
            for c in range(0, d, LANES):
                squares = squares + total[r : r + 8, c : c + LANES]
        own_squares[...] = squares

    def move(p, way, age):
        last = 2 * (n - 1)

        @pl.when(age == 0)
        def _():
            copy_of(p, way, age, "sum").start()

        @pl.when((age >= 1) & (age <= n - 1))
        def _():
            arrived(p, way, age - 1, "sum")

            @pl.when(age < n - 1)
            def _():
                add(p, way, age)
                copy_of(p, way, age, "sum").start()

            @pl.when(age == n - 1)
            def _():
                finish(p, way)

        @pl.when(age == n)
        def _():
            arrived(p, way, age - 1, "first")

        @pl.when((age > n) & (age <= last))
        def _():
            arrived(p, way, age - 1, "whole")

        @pl.when((age >= n) & (age < last))
        def _():
            copy_of(p, way, age, "whole").start()

        @pl.when(age == last)
        def _():
            keep(p, way).wait()

    in_flight = -(-(2 * (n - 1) + 1) // SLOTS)

    def slot(s):
        def one(k, _):
            q = in_flight - 1 - k
            p, age = s // SLOTS - 1 - q, s % SLOTS + SLOTS * q

            @pl.when((p >= 0) & (p < pieces))
            def _():
                @pl.when(p != pieces - 1)
                def _():
                    move(p, 0, age)

                @pl.when(p != per_layer - 1)
                def _():
                    move(p, 1, age)

            return 0

        lax.fori_loop(0, in_flight, one, 0)

    def compute(layer, p, lo, wide, last):
        units = wide * LANES
        at_units = pl.ds(lo, units)
        a_ref = (a0, a1)[layer]
        acc[...] = jnp.zeros_like(acc)

        def some(i, _):
            for k in range(tiles // SLOTS):
                at = pl.ds(pl.multiple_of((i * (tiles // SLOTS) + k) * tile, tile), tile)
                w_gate, w_up, w_down = wg[layer, :, at_units], wu[layer, :, at_units], wd[layer, at_units, :]
                a, back = a_ref[at], dh[at]
                gate, up = nn(a, w_gate), nn(a, w_up)
                by_act = nt(back, w_down).astype(BF16).astype(F32)
                s = sigmoid(gate)
                silu = gate * s
                act = (silu * up).astype(BF16)
                by_up = (by_act * silu).astype(BF16)
                by_gate = (by_act * up * (s + silu * (1.0 - s))).astype(BF16)
                acc[0:units] += tn(act, back)
                acc[units : 2 * units] += tn(by_gate, a)
                acc[2 * units : 3 * units] += tn(by_up, a)
                if layer == 1:
                    total = da[at] + nt(by_gate, w_gate) + nt(by_up, w_up)
                    if last:
                        dh[at] = (back.astype(F32) + normed_back(h1[at], total).astype(F32)).astype(BF16)
                    else:
                        da[at] = total
            slot(p * SLOTS + i)
            return 0

        lax.fori_loop(0, SLOTS, some, 0)
        for half in range(wide):
            way = half if wide == WIDE else 1 - layer
            for kind in range(KINDS):
                first = kind * units + half * LANES
                part[WIDE * p + way, kind * LANES : (kind + 1) * LANES] = acc[first : first + LANES].astype(BF16)

    def chunk_of(layer, j, _):
        base = (1 - layer) * per_layer
        compute(layer, base + j, pl.multiple_of(j * WIDE * LANES, WIDE * LANES), WIDE, False)
        return 0

    for layer in (1, 0):
        lax.fori_loop(0, per_layer - 1, functools.partial(chunk_of, layer), 0)
        compute(layer, (2 - layer) * per_layer - 1, (blocks - 1) * LANES, 1, True)

    def rest(s, _):
        slot(s)
        return 0

    done = SLOTS * (pieces + 1) + 2 * (n - 1) + 1
    summed = SLOTS * (pieces + 1) - SLOTS + n + SLOTS
    lax.fori_loop(SLOTS * pieces, summed, rest, 0)

    def squares_to(away):
        return pltpu.make_async_remote_copy(
            src_ref=own_squares,
            dst_ref=all_squares.at[me],
            send_sem=sq_send.at[away],
            recv_sem=sq_recv.at[away],
            device_id={"dp": lax.rem(me + away, n)},
            device_id_type=MESH,
        )

    def squares_from(away):
        return pltpu.make_async_remote_copy(
            src_ref=own_squares,
            dst_ref=all_squares.at[lax.rem(me - away + n, n)],
            send_sem=sq_send.at[away],
            recv_sem=sq_recv.at[away],
            device_id={"dp": lax.rem(me + away, n)},
            device_id_type=MESH,
        )

    for away in range(1, n):
        squares_to(away).start()
    all_squares[me] = own_squares[...]
    lax.fori_loop(summed, done, rest, 0)
    for away in range(1, n):
        squares_to(away).wait_send()
        squares_from(away).wait_recv()
    total = all_squares[0]
    for i in range(1, n):
        total = total + all_squares[i]
    squares_ref[...] = total


def gradients(n, tiles, x, dy, w_gate, w_up, w_down):
    (tokens, d), (layers, _, ff) = x.shape, w_gate.shape
    blocks = 2 * WIDE * ((ff // LANES + 1) // WIDE)
    rows = KINDS * LANES // n
    states = pltpu.VMEM((tokens, d), BF16)
    dma = pltpu.SemaphoreType.DMA
    any_space = pl.BlockSpec(memory_space=pl.ANY)
    return pl.pallas_call(
        functools.partial(gradients_kernel, n),
        out_shape=(
            jax.ShapeDtypeStruct((blocks, KINDS * LANES, d), BF16),
            jax.ShapeDtypeStruct((8, LANES), F32),
        ),
        in_specs=[any_space] * 5,
        out_specs=(any_space, pl.BlockSpec(memory_space=pltpu.VMEM)),
        scratch_shapes=[
            states, states, states, states,
            pltpu.VMEM(w_gate.shape, BF16), pltpu.VMEM(w_up.shape, BF16), pltpu.VMEM(w_down.shape, BF16),
            pltpu.VMEM((tokens, d), F32),
            pltpu.VMEM((KINDS * WIDE * LANES, d), F32),
            pltpu.VMEM((blocks, KINDS * LANES, d), BF16),
            pltpu.VMEM((blocks, n - 1, rows, d), BF16),
            pltpu.VMEM((8, LANES), F32),
            pltpu.VMEM((n, 8, LANES), F32),
            dma((tiles,)), dma((tiles,)), dma((layers, KINDS)),
            dma((blocks,)), dma((blocks, 2 * (n - 1))), dma((blocks,)),
            dma((n,)), dma((n,)),
        ],
        compiler_params=pltpu.CompilerParams(
            collective_id=0, has_side_effects=True, vmem_limit_bytes=67_043_328
        ),
        name="gradients",
    )(x, dy, w_gate, w_up, w_down)


def step_kernel(count, squares_ref, g1_ref, g0_ref, *refs):
    old, new = refs[:9], refs[9:]
    mean = jnp.sum(jnp.sum(squares_ref[...], 0, keepdims=True), 1, keepdims=True) / count
    factor = jnp.minimum(1.0, 0.5 * lax.rsqrt(mean + 1e-30))
    for i, kind in enumerate((1, 2, 0)):
        for layer, g_ref in ((0, g0_ref), (1, g1_ref)):
            g = g_ref[0, kind * LANES : (kind + 1) * LANES, :].astype(F32)
            if kind:
                g = g.T
            g = g * factor
            m = 0.9 * old[3 + i][layer] + 0.1 * g
            v = 0.95 * old[6 + i][layer] + 0.05 * g * g
            w = old[i][layer].astype(F32)
            new[i][layer] = (w - 0.02 * (m * lax.rsqrt(v + 1e-8) + 0.1 * w)).astype(BF16)
            new[3 + i][layer] = m
            new[6 + i][layer] = v


def take_step(summed, squares, weights, m, v):
    layers, d, ff = weights[0].shape
    blocks = ff // LANES
    count = float(sum(w.size for w in weights))
    by_columns = pl.BlockSpec((layers, d, LANES), lambda f: (0, 0, f))
    by_rows = pl.BlockSpec((layers, LANES, d), lambda f: (0, f, 0))
    arrays = [by_columns, by_columns, by_rows] * 3
    block = (1, KINDS * LANES, d)
    half = summed.shape[0] // 2
    return pl.pallas_call(
        functools.partial(step_kernel, count),
        grid=(blocks,),
        out_shape=[jax.ShapeDtypeStruct(a.shape, a.dtype) for a in (*weights, *m, *v)],
        in_specs=[
            pl.BlockSpec((8, LANES), lambda f: (0, 0)),
            pl.BlockSpec(block, lambda f: (f, 0, 0)),
            pl.BlockSpec(block, lambda f: (half + f + f // (blocks - 1), 0, 0)),
            *arrays,
        ],
        out_specs=arrays,
        compiler_params=pltpu.CompilerParams(dimension_semantics=("arbitrary",), vmem_limit_bytes=50_000_000),
        name="step",
    )(squares, summed, summed, *weights, *m, *v)


def solution(mesh, tiles=8):
    n = mesh.shape["dp"]

    def step(x, dy, *arrays):
        weights, m, v = (arrays[i : i + 3] for i in (0, 3, 6))
        summed, squares = gradients(n, tiles, x[0], dy[0], *weights)
        return tuple(take_step(summed, squares, weights, m, v))

    return jax.shard_map(
        step,
        mesh=mesh,
        in_specs=(P(("rep", "dp"), None, None),) * 2 + (P(None, None, None),) * 9,
        out_specs=(P("rep", None, None),) * 9,
        check_vma=False,
    )
```

```python
import functools

import jax
import jax.numpy as jnp
from jax import lax
from jax.experimental import pallas as pl
from jax.experimental.pallas import tpu as pltpu
from jax.sharding import PartitionSpec as P

MESH = pl.DeviceIdType.MESH
LANES = 128
KINDS = 3
WIDE = 2
SLOTS = (2, 2)
PAIR = 2
F32, BF16 = jnp.float32, jnp.bfloat16


def nn(a, b):
    return lax.dot_general(a, b, (((1,), (0,)), ((), ())), preferred_element_type=F32)


def nt(a, b):
    return lax.dot_general(a, b, (((1,), (1,)), ((), ())), preferred_element_type=F32)


def tn(a, b):
    return lax.dot_general(a, b, (((0,), (0,)), ((), ())), preferred_element_type=F32)


def sigmoid(x):
    return 0.5 * jnp.tanh(0.5 * x) + 0.5


def normed(h):
    wide = h.astype(F32)
    scale = lax.rsqrt(jnp.mean(wide * wide, -1, keepdims=True) + 1e-6)
    return (wide * scale).astype(BF16)


def normed_back(h, da):
    wide, da = h.astype(F32), da.astype(BF16).astype(F32)
    scale = lax.rsqrt(jnp.mean(wide * wide, -1, keepdims=True) + 1e-6)
    return (scale * (da - wide * (scale * scale * jnp.mean(da * wide, -1, keepdims=True)))).astype(BF16)


def gradients_kernel(
    n, x_hbm, dy_hbm, wg_hbm, wu_hbm, wd_hbm, g_hbm, squares_ref,
    a0, h1, a1, dh, wg, wu, wd, da, acc, part, recv, own_squares, all_squares,
    load_x, load_dy, load_w, send_sem, recv_sem, keep_sem, sq_send, sq_recv,
):
    tokens, d = x_hbm.shape
    ff = wg.shape[-1]
    blocks = ff // LANES
    per_layer = (blocks + 1) // WIDE
    pieces = 2 * per_layer
    rows = KINDS * LANES // n
    tiles = load_x.shape[0]
    tile = tokens // tiles
    me = lax.axis_index("dp")

    def load_tile(hbm, ref, sem, i):
        at = pl.ds(pl.multiple_of(i * tile, tile), tile)
        return pltpu.make_async_copy(hbm.at[at], ref.at[at], sem.at[i])

    def load_weight(i, layer):
        hbm, ref = ((wg_hbm, wg), (wu_hbm, wu), (wd_hbm, wd))[i]
        return pltpu.make_async_copy(hbm.at[layer], ref.at[layer], load_w.at[layer, i])

    load_tile(x_hbm, a0, load_x, 0).start()
    for i in range(KINDS):
        load_weight(i, 0).start()
    for i in range(1, tiles):
        load_tile(x_hbm, a0, load_x, i).start()
    for i in range(KINDS):
        load_weight(i, 1).start()
    for i in range(tiles):
        load_tile(dy_hbm, dh, load_dy, i).start()

    barrier = pltpu.get_barrier_semaphore()
    for away in range(1, n):
        pl.semaphore_signal(barrier, inc=1, device_id={"dp": lax.rem(me + away, n)}, device_id_type=MESH)

    own_squares[...] = jnp.zeros_like(own_squares)

    for i in range(KINDS):
        load_weight(i, 0).wait()
    bounds = [(f, min(f + 2 * LANES, ff)) for f in range(0, ff, 2 * LANES)]

    def forward(i, _):
        load_tile(x_hbm, a0, load_x, i).wait()
        at = pl.ds(pl.multiple_of(i * tile, tile), tile)
        h = a0[at]
        a = normed(h)
        total = None
        for lo, hi in bounds:
            gate, up = nn(a, wg[0, :, lo:hi]), nn(a, wu[0, :, lo:hi])
            y = nn((gate * sigmoid(gate) * up).astype(BF16), wd[0, lo:hi, :])
            total = y if total is None else total + y
        h = (h.astype(F32) + total.astype(BF16).astype(F32)).astype(BF16)
        a0[at] = a
        h1[at] = h
        a1[at] = normed(h)
        da[at] = jnp.zeros((tile, d), F32)
        return 0

    lax.fori_loop(0, tiles, forward, 0)
    for i in range(KINDS):
        load_weight(i, 1).wait()
    for i in range(tiles):
        load_tile(dy_hbm, dh, load_dy, i).wait()

    pl.semaphore_wait(barrier, n - 1)

    long, short = n // 2, n - 1 - n // 2
    flows = ((0, long), (1, short))
    last_age = 2 * long

    def chunk(c):
        return pl.ds(pl.multiple_of(lax.rem(c + 2 * n, n) * rows, rows), rows)

    def copy_of(block, sign, flow, age, source, target):
        return pltpu.make_async_remote_copy(
            src_ref=source,
            dst_ref=target,
            send_sem=send_sem.at[block, flow],
            recv_sem=recv_sem.at[block, flow, age],
            device_id={"dp": lax.rem(me + sign + n, n)},
            device_id_type=MESH,
        )

    def sum_sent(block, sign, flow, hops, age):
        source = part.at[block, chunk(me + sign * (hops - age))]
        return copy_of(block, sign, flow, age, source, recv.at[block, flow * long + age])

    def whole_sent(block, sign, flow, hop):
        at, spare = part.at[block, chunk(me - sign * hop)], recv.at[block, flow * long]
        source, target = spare if hop == 1 else at, spare if hop == 0 else at
        return copy_of(block, sign, flow, long + hop, source, target)

    def whole_received(block, sign, flow, hop):
        at = recv.at[block, flow * long] if hop == 0 else part.at[block, chunk(me - sign * (hop + 1))]
        return copy_of(block, sign, flow, long + hop, at, at)

    def keep(p, way):
        block = WIDE * p + way
        return pltpu.make_async_copy(part.at[block], g_hbm.at[block], keep_sem.at[block])

    def move(p, way, age):
        block = WIDE * p + way

        for flow, hops in flows:
            sign = (1 - 2 * way) * (1 - 2 * flow)

            @pl.when((age >= 1) & (age <= hops))
            def _():
                copy = sum_sent(block, sign, flow, hops, age - 1)
                copy.wait_send()
                copy.wait_recv()

            @pl.when((age >= 1) & (age < hops))
            def _():
                at = chunk(me + sign * (hops - age))
                came = recv[block, flow * long + age - 1].astype(F32)
                part[block, at] = (part[block, at].astype(F32) + came).astype(BF16)

            @pl.when(age < hops)
            def _():
                sum_sent(block, sign, flow, hops, age).start()

        @pl.when(age == long)
        def _():
            total = part[block, chunk(me)].astype(F32)
            for flow, hops in flows:
                total = total + recv[block, flow * long + hops - 1].astype(F32)
            total = total.astype(BF16)
            part[block, chunk(me)] = total
            total = total.astype(F32)
            total = total * total
            squares = own_squares[...]
            for r in range(0, rows, 8):
                for c in range(0, d, LANES):
                    squares = squares + total[r : r + 8, c : c + LANES]
            own_squares[...] = squares

        for flow, hops in flows:
            sign = (1 - 2 * way) * (1 - 2 * flow)

            for hop in range(hops + 1):

                @pl.when(age == long + hop)
                def _():
                    if hop > 0:
                        whole_sent(block, sign, flow, hop - 1).wait_send()
                        whole_received(block, sign, flow, hop - 1).wait_recv()
                    if hop == 1:
                        part[block, chunk(me - sign)] = recv[block, flow * long]
                    if hop < hops:
                        whole_sent(block, sign, flow, hop).start()

        @pl.when(age == last_age)
        def _():
            keep(p, way).start()

    first_steps = SLOTS[1] * per_layer
    steps = first_steps + SLOTS[0] * per_layer

    def sets_out(p):
        return jnp.where(p < per_layer, SLOTS[1] * (p + 1), first_steps + SLOTS[0] * (p + 1 - per_layer))

    in_flight = last_age // min(SLOTS) + 1

    def slot(s, current):
        def one(k, _):
            p = current - in_flight + k
            age = s - sets_out(p)

            @pl.when((p >= 0) & (p < pieces) & (age <= last_age) & (age >= 0))
            def _():
                move(p, 0, age)

                @pl.when((p != per_layer - 1) & (p != pieces - 1))
                def _():
                    move(p, 1, age)

            return 0

        lax.fori_loop(0, in_flight, one, 0)

    def compute(layer, p, lo, wide, last):
        units = wide * LANES
        at_units = pl.ds(lo, units)
        a_ref = (a0, a1)[layer]
        acc[...] = jnp.zeros_like(acc)

        def some(i, _):
            for k in range(PAIR):
                at = pl.ds(pl.multiple_of((i * PAIR + k) * tile, tile), tile)
                w_gate, w_up, w_down = wg[layer, :, at_units], wu[layer, :, at_units], wd[layer, at_units, :]
                a, back = a_ref[at], dh[at]
                gate, up = nn(a, w_gate), nn(a, w_up)
                by_act = nt(back, w_down).astype(BF16).astype(F32)
                s = sigmoid(gate)
                silu = gate * s
                act = (silu * up).astype(BF16)
                by_up = (by_act * silu).astype(BF16)
                by_gate = (by_act * up * (s + silu * (1.0 - s))).astype(BF16)
                acc[0:units] += tn(act, back)
                acc[units : 2 * units] += tn(by_gate, a)
                acc[2 * units : 3 * units] += tn(by_up, a)
                if layer == 1:
                    total = da[at] + nt(by_gate, w_gate) + nt(by_up, w_up)
                    if last:
                        dh[at] = (back.astype(F32) + normed_back(h1[at], total).astype(F32)).astype(BF16)
                    else:
                        da[at] = total
            return 0

        between = tiles // PAIR // SLOTS[layer]
        before = sets_out(p) - SLOTS[layer]

        def stretch(i, _):
            lax.fori_loop(i * between, (i + 1) * between, some, 0)
            slot(before + i, p)
            return 0

        lax.fori_loop(0, SLOTS[layer], stretch, 0)
        for half in range(wide):
            for kind in range(KINDS):
                first = kind * units + half * LANES
                part[WIDE * p + half, kind * LANES : (kind + 1) * LANES] = acc[first : first + LANES].astype(BF16)

    def chunk_of(layer, j, _):
        base = (1 - layer) * per_layer
        compute(layer, base + j, pl.multiple_of(j * WIDE * LANES, WIDE * LANES), WIDE, False)
        return 0

    for layer in (1, 0):
        lax.fori_loop(0, per_layer - 1, functools.partial(chunk_of, layer), 0)
        compute(layer, (2 - layer) * per_layer - 1, (blocks - 1) * LANES, 1, True)

    def rest(s, _):
        slot(s, pieces)
        return 0

    lax.fori_loop(steps, steps + long + 1, rest, 0)

    def squares_to(away):
        return pltpu.make_async_remote_copy(
            src_ref=own_squares,
            dst_ref=all_squares.at[me],
            send_sem=sq_send.at[away],
            recv_sem=sq_recv.at[away],
            device_id={"dp": lax.rem(me + away, n)},
            device_id_type=MESH,
        )

    def squares_from(away):
        return pltpu.make_async_remote_copy(
            src_ref=own_squares,
            dst_ref=all_squares.at[lax.rem(me - away + n, n)],
            send_sem=sq_send.at[away],
            recv_sem=sq_recv.at[away],
            device_id={"dp": lax.rem(me + away, n)},
            device_id_type=MESH,
        )

    for away in range(1, n):
        squares_to(away).start()
    all_squares[me] = own_squares[...]
    lax.fori_loop(steps + long + 1, steps + last_age + 1, rest, 0)
    for away in range(1, n):
        squares_to(away).wait_send()
        squares_from(away).wait_recv()
    total = all_squares[0]
    for i in range(1, n):
        total = total + all_squares[i]
    squares_ref[...] = total

    def kept(block, _):
        @pl.when((block != WIDE * per_layer - 1) & (block != WIDE * pieces - 1))
        def _():
            keep(0, block).wait()

        return 0

    lax.fori_loop(0, WIDE * pieces, kept, 0)


def gradients(n, tiles, x, dy, w_gate, w_up, w_down):
    (tokens, d), (layers, _, ff) = x.shape, w_gate.shape
    blocks = 2 * WIDE * ((ff // LANES + 1) // WIDE)
    rows = KINDS * LANES // n
    states = pltpu.VMEM((tokens, d), BF16)
    dma = pltpu.SemaphoreType.DMA
    any_space = pl.BlockSpec(memory_space=pl.ANY)
    return pl.pallas_call(
        functools.partial(gradients_kernel, n),
        out_shape=(
            jax.ShapeDtypeStruct((blocks, KINDS * LANES, d), BF16),
            jax.ShapeDtypeStruct((8, LANES), F32),
        ),
        in_specs=[any_space] * 5,
        out_specs=(any_space, pl.BlockSpec(memory_space=pltpu.VMEM)),
        scratch_shapes=[
            states, states, states, states,
            pltpu.VMEM(w_gate.shape, BF16), pltpu.VMEM(w_up.shape, BF16), pltpu.VMEM(w_down.shape, BF16),
            pltpu.VMEM((tokens, d), F32),
            pltpu.VMEM((KINDS * WIDE * LANES, d), F32),
            pltpu.VMEM((blocks, KINDS * LANES, d), BF16),
            pltpu.VMEM((blocks, n - 1, rows, d), BF16),
            pltpu.VMEM((8, LANES), F32),
            pltpu.VMEM((n, 8, LANES), F32),
            dma((tiles,)), dma((tiles,)), dma((layers, KINDS)),
            dma((blocks, 2)), dma((blocks, 2, 2 * (n // 2))), dma((blocks,)),
            dma((n,)), dma((n,)),
        ],
        compiler_params=pltpu.CompilerParams(
            collective_id=0, has_side_effects=True, vmem_limit_bytes=67_043_328
        ),
        name="gradients",
    )(x, dy, w_gate, w_up, w_down)


def step_kernel(count, squares_ref, g_ref, *refs):
    old, new = refs[:9], refs[9:]
    mean = jnp.sum(jnp.sum(squares_ref[...], 0, keepdims=True), 1, keepdims=True) / count
    factor = jnp.minimum(1.0, 0.5 * lax.rsqrt(mean + 1e-30))
    for i, kind in enumerate((1, 2, 0)):
        for half in range(WIDE):
            g = g_ref[half, kind * LANES : (kind + 1) * LANES, :].astype(F32)
            units = slice(half * LANES, (half + 1) * LANES)
            at = (0, slice(None), units) if kind else (0, units)
            g = (g.T if kind else g) * factor
            m = 0.9 * old[3 + i][at] + 0.1 * g
            v = 0.95 * old[6 + i][at] + 0.05 * g * g
            w = old[i][at].astype(F32)
            new[i][at] = (w - 0.02 * (m * lax.rsqrt(v + 1e-8) + 0.1 * w)).astype(BF16)
            new[3 + i][at] = m
            new[6 + i][at] = v


def take_step(summed, squares, weights, m, v):
    layers, d, ff = weights[0].shape
    units = WIDE * LANES
    pieces = pl.cdiv(ff, units)
    count = float(sum(w.size for w in weights))
    by_columns = pl.BlockSpec((1, d, units), lambda layer, j: (layer, 0, j))
    by_rows = pl.BlockSpec((1, units, d), lambda layer, j: (layer, j, 0))
    arrays = [by_columns, by_columns, by_rows] * 3
    return pl.pallas_call(
        functools.partial(step_kernel, count),
        grid=(layers, pieces),
        out_shape=[jax.ShapeDtypeStruct(a.shape, a.dtype) for a in (*weights, *m, *v)],
        in_specs=[
            pl.BlockSpec((8, LANES), lambda layer, j: (0, 0)),
            pl.BlockSpec((WIDE, KINDS * LANES, d), lambda layer, j: ((layers - 1 - layer) * pieces + j, 0, 0)),
            *arrays,
        ],
        out_specs=arrays,
        compiler_params=pltpu.CompilerParams(
            dimension_semantics=("arbitrary", "arbitrary"), vmem_limit_bytes=67_043_328
        ),
        name="step",
    )(squares, summed, *weights, *m, *v)


def solution(mesh, tiles=8):
    n = mesh.shape["dp"]

    def step(x, dy, *arrays):
        weights, m, v = (arrays[i : i + 3] for i in (0, 3, 6))
        summed, squares = gradients(n, tiles, x[0], dy[0], *weights)
        return tuple(take_step(summed, squares, weights, m, v))

    return jax.shard_map(
        step,
        mesh=mesh,
        in_specs=(P(("rep", "dp"), None, None),) * 2 + (P(None, None, None),) * 9,
        out_specs=(P("rep", None, None),) * 9,
        check_vma=False,
    )
```

```python
import functools

import jax
import jax.numpy as jnp
from jax import lax
from jax.experimental import pallas as pl
from jax.experimental.pallas import tpu as pltpu
from jax.sharding import PartitionSpec as P

MESH = pl.DeviceIdType.MESH
LANES = 128
KINDS = 3
WIDE = 2
SLOTS = (2, 2)
PAIR = 2
F32, BF16 = jnp.float32, jnp.bfloat16


def nn(a, b):
    return lax.dot_general(a, b, (((1,), (0,)), ((), ())), preferred_element_type=F32)


def nt(a, b):
    return lax.dot_general(a, b, (((1,), (1,)), ((), ())), preferred_element_type=F32)


def tn(a, b):
    return lax.dot_general(a, b, (((0,), (0,)), ((), ())), preferred_element_type=F32)


def sigmoid(x):
    return 0.5 * jnp.tanh(0.5 * x) + 0.5


def normed(h):
    wide = h.astype(F32)
    scale = lax.rsqrt(jnp.mean(wide * wide, -1, keepdims=True) + 1e-6)
    return (wide * scale).astype(BF16)


def normed_back(h, da):
    wide, da = h.astype(F32), da.astype(BF16).astype(F32)
    scale = lax.rsqrt(jnp.mean(wide * wide, -1, keepdims=True) + 1e-6)
    return (scale * (da - wide * (scale * scale * jnp.mean(da * wide, -1, keepdims=True)))).astype(BF16)


def gradients_kernel(
    n, x_hbm, dy_hbm, wg_hbm, wu_hbm, wd_hbm, g_hbm, squares_ref,
    a0, h1, a1, dh, wg, wu, wd, da, acc, part, recv, own_squares, all_squares,
    load_x, load_dy, load_w, send_sem, recv_sem, keep_sem, sq_send, sq_recv,
):
    tokens, d = x_hbm.shape
    ff = wg.shape[-1]
    blocks = ff // LANES
    per_layer = (blocks + 1) // WIDE
    pieces = 2 * per_layer
    rows = KINDS * LANES // n
    tiles = load_x.shape[0]
    tile = tokens // tiles
    me = lax.axis_index("dp")

    def load_tile(hbm, ref, sem, i):
        at = pl.ds(pl.multiple_of(i * tile, tile), tile)
        return pltpu.make_async_copy(hbm.at[at], ref.at[at], sem.at[i])

    def load_weight(i, layer):
        hbm, ref = ((wg_hbm, wg), (wu_hbm, wu), (wd_hbm, wd))[i]
        return pltpu.make_async_copy(hbm.at[layer], ref.at[layer], load_w.at[layer, i])

    load_tile(x_hbm, a0, load_x, 0).start()
    for i in range(KINDS):
        load_weight(i, 0).start()
    for i in range(1, tiles):
        load_tile(x_hbm, a0, load_x, i).start()
    for i in range(KINDS):
        load_weight(i, 1).start()
    for i in range(tiles):
        load_tile(dy_hbm, dh, load_dy, i).start()

    barrier = pltpu.get_barrier_semaphore()
    for away in range(1, n):
        pl.semaphore_signal(barrier, inc=1, device_id={"dp": lax.rem(me + away, n)}, device_id_type=MESH)

    own_squares[...] = jnp.zeros_like(own_squares)

    for i in range(KINDS):
        load_weight(i, 0).wait()
    bounds = [(f, min(f + 2 * LANES, ff)) for f in range(0, ff, 2 * LANES)]

    def forward(i, _):
        load_tile(x_hbm, a0, load_x, i).wait()
        at = pl.ds(pl.multiple_of(i * tile, tile), tile)
        h = a0[at]
        a = normed(h)
        total = None
        for lo, hi in bounds:
            gate, up = nn(a, wg[0, :, lo:hi]), nn(a, wu[0, :, lo:hi])
            y = nn((gate * sigmoid(gate) * up).astype(BF16), wd[0, lo:hi, :])
            total = y if total is None else total + y
        h = (h.astype(F32) + total.astype(BF16).astype(F32)).astype(BF16)
        a0[at] = a
        h1[at] = h
        a1[at] = normed(h)
        da[at] = jnp.zeros((tile, d), F32)
        return 0

    lax.fori_loop(0, tiles, forward, 0)
    for i in range(KINDS):
        load_weight(i, 1).wait()
    for i in range(tiles):
        load_tile(dy_hbm, dh, load_dy, i).wait()

    pl.semaphore_wait(barrier, n - 1)

    long, short = n // 2, n - 1 - n // 2
    flows = ((0, long), (1, short))
    last_age = 2 * long

    def chunk(c):
        return pl.ds(pl.multiple_of(lax.rem(c + 2 * n, n) * rows, rows), rows)

    def copy_of(block, sign, flow, age, source, target):
        return pltpu.make_async_remote_copy(
            src_ref=source,
            dst_ref=target,
            send_sem=send_sem.at[block, flow],
            recv_sem=recv_sem.at[block, flow, age],
            device_id={"dp": lax.rem(me + sign + n, n)},
            device_id_type=MESH,
        )

    def sum_sent(block, sign, flow, hops, age):
        source = part.at[block, chunk(me + sign * (hops - age))]
        return copy_of(block, sign, flow, age, source, recv.at[block, flow * long + age])

    def whole_sent(block, sign, flow, hop):
        at, spare = part.at[block, chunk(me - sign * hop)], recv.at[block, flow * long]
        source, target = spare if hop == 1 else at, spare if hop == 0 else at
        return copy_of(block, sign, flow, long + hop, source, target)

    def whole_received(block, sign, flow, hop):
        at = recv.at[block, flow * long] if hop == 0 else part.at[block, chunk(me - sign * (hop + 1))]
        return copy_of(block, sign, flow, long + hop, at, at)

    def keep(p, way):
        block = WIDE * p + way
        return pltpu.make_async_copy(part.at[block], g_hbm.at[block], keep_sem.at[block])

    def move(p, way, age):
        block = WIDE * p + way

        for flow, hops in flows:
            sign = (1 - 2 * way) * (1 - 2 * flow)

            @pl.when((age >= 1) & (age <= hops))
            def _():
                copy = sum_sent(block, sign, flow, hops, age - 1)
                copy.wait_send()
                copy.wait_recv()

            @pl.when((age >= 1) & (age < hops))
            def _():
                at = chunk(me + sign * (hops - age))
                came = recv[block, flow * long + age - 1].astype(F32)
                part[block, at] = (part[block, at].astype(F32) + came).astype(BF16)

            @pl.when(age < hops)
            def _():
                sum_sent(block, sign, flow, hops, age).start()

        @pl.when(age == long)
        def _():
            total = part[block, chunk(me)].astype(F32)
            for flow, hops in flows:
                total = total + recv[block, flow * long + hops - 1].astype(F32)
            total = total.astype(BF16)
            part[block, chunk(me)] = total
            total = total.astype(F32)
            total = total * total
            squares = own_squares[...]
            for r in range(0, rows, 8):
                for c in range(0, d, LANES):
                    squares = squares + total[r : r + 8, c : c + LANES]
            own_squares[...] = squares

        for flow, hops in flows:
            sign = (1 - 2 * way) * (1 - 2 * flow)

            for hop in range(hops + 1):

                @pl.when(age == long + hop)
                def _():
                    if hop > 0:
                        whole_sent(block, sign, flow, hop - 1).wait_send()
                        whole_received(block, sign, flow, hop - 1).wait_recv()
                    if hop == 1:
                        part[block, chunk(me - sign)] = recv[block, flow * long]
                    if hop < hops:
                        whole_sent(block, sign, flow, hop).start()

        @pl.when(age == last_age)
        def _():
            keep(p, way).start()

    first_steps = SLOTS[1] * (per_layer + 1)
    steps = first_steps + SLOTS[0] * per_layer

    def sets_out(p):
        return jnp.where(p < per_layer, SLOTS[1] * (p + 1 + jnp.minimum(p, 1)), first_steps + SLOTS[0] * (p + 1 - per_layer))

    in_flight = last_age // min(SLOTS) + 1

    def slot(s, current):
        def one(k, _):
            p = current - in_flight + k
            age = s - sets_out(p)

            @pl.when((p >= 0) & (p < pieces) & (age <= last_age) & (age >= 0))
            def _():
                move(p, 0, age)

                @pl.when((p != per_layer - 1) & (p != pieces - 1))
                def _():
                    move(p, 1, age)

            return 0

        lax.fori_loop(0, in_flight, one, 0)

    def compute(layer, p, lo, wide, last):
        units = wide * LANES
        at_units = pl.ds(lo, units)
        a_ref = (a0, a1)[layer]
        acc[...] = jnp.zeros_like(acc)

        def some(i, _):
            for k in range(PAIR):
                at = pl.ds(pl.multiple_of((i * PAIR + k) * tile, tile), tile)
                w_gate, w_up, w_down = wg[layer, :, at_units], wu[layer, :, at_units], wd[layer, at_units, :]
                a, back = a_ref[at], dh[at]
                gate, up = nn(a, w_gate), nn(a, w_up)
                by_act = nt(back, w_down).astype(BF16).astype(F32)
                s = sigmoid(gate)
                silu = gate * s
                act = (silu * up).astype(BF16)
                by_up = (by_act * silu).astype(BF16)
                by_gate = (by_act * up * (s + silu * (1.0 - s))).astype(BF16)
                acc[0:units] += tn(act, back)
                acc[units : 2 * units] += tn(by_gate, a)
                acc[2 * units : 3 * units] += tn(by_up, a)
                if layer == 1:
                    total = da[at] + nt(by_gate, w_gate) + nt(by_up, w_up)
                    if last:
                        dh[at] = (back.astype(F32) + normed_back(h1[at], total).astype(F32)).astype(BF16)
                    else:
                        da[at] = total
            return 0

        count = SLOTS[layer] * (1 + (p == 1)) if layer == 1 else SLOTS[layer]
        between = tiles // PAIR // count
        before = sets_out(p) - count

        def stretch(i, _):
            slot(before + i, p)
            lax.fori_loop(i * between, (i + 1) * between, some, 0)
            return 0

        lax.fori_loop(0, count, stretch, 0)
        for half in range(wide):
            for kind in range(KINDS):
                first = kind * units + half * LANES
                part[WIDE * p + half, kind * LANES : (kind + 1) * LANES] = acc[first : first + LANES].astype(BF16)

    def chunk_of(layer, j, _):
        base = (1 - layer) * per_layer
        compute(layer, base + j, pl.multiple_of(j * WIDE * LANES, WIDE * LANES), WIDE, False)
        return 0

    for layer in (1, 0):
        lax.fori_loop(0, per_layer - 1, functools.partial(chunk_of, layer), 0)
        compute(layer, (2 - layer) * per_layer - 1, (blocks - 1) * LANES, 1, True)

    def rest(s, _):
        slot(s, pieces)
        return 0

    lax.fori_loop(steps, steps + long + 1, rest, 0)

    def squares_to(away):
        return pltpu.make_async_remote_copy(
            src_ref=own_squares,
            dst_ref=all_squares.at[me],
            send_sem=sq_send.at[away],
            recv_sem=sq_recv.at[away],
            device_id={"dp": lax.rem(me + away, n)},
            device_id_type=MESH,
        )

    def squares_from(away):
        return pltpu.make_async_remote_copy(
            src_ref=own_squares,
            dst_ref=all_squares.at[lax.rem(me - away + n, n)],
            send_sem=sq_send.at[away],
            recv_sem=sq_recv.at[away],
            device_id={"dp": lax.rem(me + away, n)},
            device_id_type=MESH,
        )

    for away in range(1, n):
        squares_to(away).start()
    all_squares[me] = own_squares[...]
    lax.fori_loop(steps + long + 1, steps + last_age + 1, rest, 0)
    for away in range(1, n):
        squares_to(away).wait_send()
        squares_from(away).wait_recv()
    total = all_squares[0]
    for i in range(1, n):
        total = total + all_squares[i]
    squares_ref[...] = total

    def kept(block, _):
        @pl.when((block != WIDE * per_layer - 1) & (block != WIDE * pieces - 1))
        def _():
            keep(0, block).wait()

        return 0

    lax.fori_loop(0, WIDE * pieces, kept, 0)


def gradients(n, tiles, x, dy, w_gate, w_up, w_down):
    (tokens, d), (layers, _, ff) = x.shape, w_gate.shape
    blocks = 2 * WIDE * ((ff // LANES + 1) // WIDE)
    rows = KINDS * LANES // n
    states = pltpu.VMEM((tokens, d), BF16)
    dma = pltpu.SemaphoreType.DMA
    any_space = pl.BlockSpec(memory_space=pl.ANY)
    return pl.pallas_call(
        functools.partial(gradients_kernel, n),
        out_shape=(
            jax.ShapeDtypeStruct((blocks, KINDS * LANES, d), BF16),
            jax.ShapeDtypeStruct((8, LANES), F32),
        ),
        in_specs=[any_space] * 5,
        out_specs=(any_space, pl.BlockSpec(memory_space=pltpu.VMEM)),
        scratch_shapes=[
            states, states, states, states,
            pltpu.VMEM(w_gate.shape, BF16), pltpu.VMEM(w_up.shape, BF16), pltpu.VMEM(w_down.shape, BF16),
            pltpu.VMEM((tokens, d), F32),
            pltpu.VMEM((KINDS * WIDE * LANES, d), F32),
            pltpu.VMEM((blocks, KINDS * LANES, d), BF16),
            pltpu.VMEM((blocks, n - 1, rows, d), BF16),
            pltpu.VMEM((8, LANES), F32),
            pltpu.VMEM((n, 8, LANES), F32),
            dma((tiles,)), dma((tiles,)), dma((layers, KINDS)),
            dma((blocks, 2)), dma((blocks, 2, 2 * (n // 2))), dma((blocks,)),
            dma((n,)), dma((n,)),
        ],
        compiler_params=pltpu.CompilerParams(
            collective_id=0, has_side_effects=True, vmem_limit_bytes=67_043_328
        ),
        name="gradients",
    )(x, dy, w_gate, w_up, w_down)


def step_kernel(count, squares_ref, g_ref, *refs):
    old, new = refs[:9], refs[9:]
    mean = jnp.sum(jnp.sum(squares_ref[...], 0, keepdims=True), 1, keepdims=True) / count
    factor = jnp.minimum(1.0, 0.5 * lax.rsqrt(mean + 1e-30))
    for i, kind in enumerate((1, 2, 0)):
        for half in range(WIDE):
            g = g_ref[half, kind * LANES : (kind + 1) * LANES, :].astype(F32)
            units = slice(half * LANES, (half + 1) * LANES)
            at = (0, slice(None), units) if kind else (0, units)
            g = (g.T if kind else g) * factor
            m = 0.9 * old[3 + i][at] + 0.1 * g
            v = 0.95 * old[6 + i][at] + 0.05 * g * g
            w = old[i][at].astype(F32)
            new[i][at] = (w - 0.02 * (m * lax.rsqrt(v + 1e-8) + 0.1 * w)).astype(BF16)
            new[3 + i][at] = m
            new[6 + i][at] = v


def take_step(summed, squares, weights, m, v):
    layers, d, ff = weights[0].shape
    units = WIDE * LANES
    pieces = pl.cdiv(ff, units)
    count = float(sum(w.size for w in weights))
    by_columns = pl.BlockSpec((1, d, units), lambda layer, j: (layer, 0, j))
    by_rows = pl.BlockSpec((1, units, d), lambda layer, j: (layer, j, 0))
    arrays = [by_columns, by_columns, by_rows] * 3
    return pl.pallas_call(
        functools.partial(step_kernel, count),
        grid=(layers, pieces),
        out_shape=[jax.ShapeDtypeStruct(a.shape, a.dtype) for a in (*weights, *m, *v)],
        in_specs=[
            pl.BlockSpec((8, LANES), lambda layer, j: (0, 0)),
            pl.BlockSpec((WIDE, KINDS * LANES, d), lambda layer, j: ((layers - 1 - layer) * pieces + j, 0, 0)),
            *arrays,
        ],
        out_specs=arrays,
        compiler_params=pltpu.CompilerParams(
            dimension_semantics=("arbitrary", "arbitrary"), vmem_limit_bytes=67_043_328
        ),
        name="step",
    )(squares, summed, *weights, *m, *v)


def solution(mesh, tiles=8):
    n = mesh.shape["dp"]

    def step(x, dy, *arrays):
        weights, m, v = (arrays[i : i + 3] for i in (0, 3, 6))
        summed, squares = gradients(n, tiles, x[0], dy[0], *weights)
        return tuple(take_step(summed, squares, weights, m, v))

    return jax.shard_map(
        step,
        mesh=mesh,
        in_specs=(P(("rep", "dp"), None, None),) * 2 + (P(None, None, None),) * 9,
        out_specs=(P("rep", None, None),) * 9,
        check_vma=False,
    )
```
